32 devices in a mesh: lat: 2 (over x), lon: 4 (over y, core), lev: 4 (over z).
Axes of the slice: x: 2, y: 2, z: 4, core: 2. Of those that a mesh axis runs over, the one named last changes fastest.
Arguments:
- initial_state: float32 [16, 128, 256, 128], P('lat', 'lon', 'lev'), may hold values from 0.2 to 1.8
- scaled_diffusivity: float32 [16, 128, 256, 128], P('lat', 'lon', 'lev'), may hold values from 0.03 to 0.15
- scaled_forcing: float32 [16, 128, 256, 128], P('lat', 'lon', 'lev'), may hold values from -0.2 to 0.2
Outputs:
- cumulative_totals: float32 [16, 128, 256, 128], P('lat', 'lon', 'lev')
- temperature_end: float32 [16, 128, 256, 128], P('lat', 'lon', 'lev')
The draws below stay inside these ranges and needn't reach their ends.
All inputs are finite; a program needn't handle non-finite values.
Results may differ from the reference program's by a relative error of at most 0.00002.
Values sent between devices are 32-bit elements; how exact they have to be, the bound alone decides.
A program may use at most 128 MiB of HBM per device.

```python
import jax
import jax.numpy as jnp
from jax import lax

SECOND_EXTENT = 16
FIRST_EXTENT = 128
THIRD_EXTENT = 256
MEMBER_TALLY = 128
STEPS = 4


def level_of(rng, extent, cuts, smallest, top_value):
    def one(axis_at, shards_of):
        draws = jax.random.uniform(jax.random.fold_in(jax.random.fold_in(rng, 6), axis_at), (shards_of,), jnp.float32, smallest / len(cuts), top_value / len(cuts))
        return jnp.repeat(jnp.exp(draws), extent[axis_at] // shards_of).reshape((-1,) + (1,) * (len(extent) - axis_at - 1))

    level = one(*cuts[0])
    for cut in cuts[1:]:
        level = level * one(*cut)
    return level


def setup_inputs(seed: int = 0) -> dict:
    seeds = jax.random.split(jax.random.key(seed), 4)
    initial_state = jnp.clip(0.2 + 1.5999999 * jax.random.uniform(seeds[0], (SECOND_EXTENT, FIRST_EXTENT, THIRD_EXTENT, MEMBER_TALLY), jnp.float32) ** level_of(seeds[0], (SECOND_EXTENT, FIRST_EXTENT, THIRD_EXTENT, MEMBER_TALLY), ((0, 2), (1, 4), (2, 4)), -0.2, 0.2), 0.2, 1.8)
    scaled_diffusivity = jnp.clip(0.03 + 0.120000007 * jax.random.uniform(seeds[1], (SECOND_EXTENT, FIRST_EXTENT, THIRD_EXTENT, MEMBER_TALLY), jnp.float32) ** level_of(seeds[1], (SECOND_EXTENT, FIRST_EXTENT, THIRD_EXTENT, MEMBER_TALLY), ((0, 2), (1, 4), (2, 4)), -0.2, 0.2), 0.03, 0.15)
    scaled_forcing = jnp.clip(jax.random.uniform(seeds[2], (SECOND_EXTENT, FIRST_EXTENT, THIRD_EXTENT, MEMBER_TALLY), jnp.float32, -0.2, 0.2) * level_of(seeds[2], (SECOND_EXTENT, FIRST_EXTENT, THIRD_EXTENT, MEMBER_TALLY), ((0, 2), (1, 4), (2, 4)), -0.4, 0.0), -0.2, 0.2)
    return dict(initial_state=initial_state, scaled_diffusivity=scaled_diffusivity, scaled_forcing=scaled_forcing)


def strip_edges(values, dims):
    for dim in dims:
        values = lax.slice_in_dim(values, 1, values.shape[dim] - 1, axis=dim)
    return values


def neighbour(values, dim, start, dims):
    others = [other for other in dims if other != dim]
    values = strip_edges(values, others)
    return lax.slice_in_dim(values, start, start + values.shape[dim] - 2, axis=dim)


def explicit_update(haloed_values, scaled_diffusivity, scaled_forcing):
    middle = strip_edges(haloed_values, (0, 1, 2))
    lower = [neighbour(haloed_values, dim, 0, (0, 1, 2)) for dim in (0, 1, 2)]
    upper = [neighbour(haloed_values, dim, 2, (0, 1, 2)) for dim in (0, 1, 2)]
    spread = lower[0] + upper[0] + lower[1] + upper[1] + lower[2] + upper[2] - 6.0 * middle
    return middle + scaled_diffusivity * spread + scaled_forcing


def reference(initial_state, scaled_diffusivity, scaled_forcing):
    for step in range(STEPS):
        initial_state = explicit_update(jnp.pad(initial_state, ((1, 1), (1, 1), (1, 1), (0, 0)), mode="constant"), scaled_diffusivity, scaled_forcing)
    cumulative_totals = jnp.cumsum(initial_state, axis=1) / FIRST_EXTENT
    return cumulative_totals, initial_state
```

```python
import functools

import jax
import jax.numpy as jnp
from jax import lax
from jax.experimental import pallas as pl
from jax.experimental.pallas import tpu as pltpu
from jax.sharding import PartitionSpec as P

STEPS = 4
PAD = 8
CHUNK = 8
MESH = pl.DeviceIdType.MESH


def steps_kernel(
    sizes, x, d, f, end, before, state, coef, source,
    lev_out, lev_in, tot_mid, tot_edge, mid_in, edge_in,
    lat_send, lat_recv, lon_send, lon_recv, lev_send, lev_recv,
    load_sem, end_sem, tot_send, tot_recv,
):
    J, I, K, M = x.shape
    chunks = K // CHUNK
    me = {axis: lax.axis_index(axis) for axis in sizes}
    n_lon = sizes["lon"]
    rows = pl.ds(1, I)
    levels = pl.ds(PAD, K)
    planes = pl.ds(1, J)

    def has(axis, side):
        return me[axis] > 0 if side == 0 else me[axis] < sizes[axis] - 1

    def beside(axis, side):
        return {axis: me[axis] - 1 if side == 0 else me[axis] + 1}

    def both(axis, act):
        if sizes[axis] > 1:
            for side in (0, 1):
                pl.when(has(axis, side))(functools.partial(act, side))

    def load(which, j):
        src, dst = (
            (x.at[j], state.at[0, j + 1, rows, levels]),
            (d.at[j], coef.at[j]),
            (f.at[j], source.at[j]),
        )[which]
        return pltpu.make_async_copy(src, dst, load_sem.at[which, j])

    for which in range(3):
        for j in range(J):
            load(which, j).start()

    barrier = pltpu.get_barrier_semaphore()
    count = jnp.int32(n_lon - 1)

    def greet(target):
        pl.semaphore_signal(barrier, inc=1, device_id=target, device_id_type=MESH)

    for axis in ("lat", "lev"):
        both(axis, lambda side, axis=axis: greet(beside(axis, side)))
        if sizes[axis] > 1:
            count = count + has(axis, 0).astype(jnp.int32) + has(axis, 1).astype(jnp.int32)
    for other in range(n_lon):
        pl.when(other != me["lon"])(lambda other=other: greet({"lon": jnp.int32(other)}))
    pl.semaphore_wait(barrier, count)

    def lat_copy(step, side, c):
        slot = step % 2
        part = pl.ds(pl.multiple_of(PAD + c * CHUNK, CHUNK), CHUNK)
        plane, target = (1, J + 1) if side == 0 else (J, 0)
        if step == 0:
            inner = pl.ds(pl.multiple_of(c * CHUNK, CHUNK), CHUNK)
            src = x.at[plane - 1, :, inner]
        else:
            src = state.at[slot, plane, rows, part]
        return pltpu.make_async_remote_copy(
            src_ref=src,
            dst_ref=state.at[slot, target, rows, part],
            send_sem=lat_send.at[slot, side, c],
            recv_sem=lat_recv.at[slot, 1 - side, c],
            device_id=beside("lat", side),
            device_id_type=MESH,
        )

    def lat_arrived(step, side, c):
        slot = step % 2
        part = pl.ds(pl.multiple_of(PAD + c * CHUNK, CHUNK), CHUNK)
        target = 0 if side == 0 else J + 1
        pltpu.make_async_remote_copy(
            src_ref=state.at[slot, target, rows, part],
            dst_ref=state.at[slot, target, rows, part],
            send_sem=lat_send.at[slot, side, c],
            recv_sem=lat_recv.at[slot, side, c],
            device_id=beside("lat", side),
            device_id_type=MESH,
        ).wait_recv()

    def lon_copy(step, side, arriving=False):
        slot = step % 2
        row, target = (1, I + 1) if side == 0 else (I, 0)
        dst = (0 if side == 0 else I + 1) if arriving else target
        return pltpu.make_async_remote_copy(
            src_ref=state.at[slot, planes, row, levels],
            dst_ref=state.at[slot, planes, dst, levels],
            send_sem=lon_send.at[slot, side],
            recv_sem=lon_recv.at[slot, side if arriving else 1 - side],
            device_id=beside("lon", side),
            device_id_type=MESH,
        )

    def lev_copy(step, side, arriving=False):
        slot = step % 2
        landing = side if arriving else 1 - side
        return pltpu.make_async_remote_copy(
            src_ref=lev_out.at[side],
            dst_ref=lev_in.at[slot, landing],
            send_sem=lev_send.at[slot, side],
            recv_sem=lev_recv.at[slot, landing],
            device_id=beside("lev", side),
            device_id_type=MESH,
        )

    def lat_start(step, c):
        both("lat", lambda side: lat_copy(step, side, c).start())

    for c in range(chunks):
        lat_start(0, c)

    def clear(axis, side):
        for slot in (0, 1):
            if axis == "lat":
                target = 0 if side == 0 else J + 1

                @pl.loop(1, I + 1)
                def _(i):
                    state[slot, target, i, PAD : PAD + K, :] = jnp.zeros((K, M), jnp.float32)
            elif axis == "lon":
                target = 0 if side == 0 else I + 1
                for p in range(1, J + 1):
                    state[slot, p, target, PAD : PAD + K, :] = jnp.zeros((K, M), jnp.float32)
            else:
                target = PAD - 1 if side == 0 else PAD + K

                @pl.loop(1, J + 1)
                def _(p):
                    state[slot, p, 1 : I + 1, target : target + 1, :] = jnp.zeros(
                        (I, 1, M), jnp.float32
                    )

    for axis in ("lat", "lon", "lev"):
        for side in (0, 1):
            pl.when(jnp.logical_not(has(axis, side)))(functools.partial(clear, axis, side))

    for j in range(J):
        load(0, j).wait()

    def update(step, p, i, start, length):
        a, b = step % 2, (step + 1) % 2
        here = pl.ds(start, length)
        inner = pl.ds(start - PAD, length)
        middle = state[a, p, i, here, :]
        spread = (
            (state[a, p - 1, i, here, :] + state[a, p + 1, i, here, :])
            + (state[a, p, i - 1, here, :] + state[a, p, i + 1, here, :])
            + (
                state[a, p, i, pl.ds(start - 1, length), :]
                + state[a, p, i, pl.ds(start + 1, length), :]
            )
            - 6.0 * middle
        )
        new = middle + coef[p - 1, i - 1, inner, :] * spread + source[p - 1, i - 1, inner, :]
        state[b, p, i, here, :] = new
        return new

    def mid_total(target, arriving=None):
        sender = me["lon"] if arriving is None else arriving
        return pltpu.make_async_remote_copy(
            src_ref=tot_mid,
            dst_ref=mid_in.at[sender],
            send_sem=tot_send.at[target, chunks],
            recv_sem=tot_recv.at[sender, chunks],
            device_id={"lon": jnp.int32(target)},
            device_id_type=MESH,
        )

    def edge_total(target, c, arriving=None):
        sender = me["lon"] if arriving is None else arriving
        part = pl.ds(pl.multiple_of(c * CHUNK, CHUNK), CHUNK)
        return pltpu.make_async_remote_copy(
            src_ref=tot_edge.at[:, part],
            dst_ref=edge_in.at[sender, :, part],
            send_sem=tot_send.at[target, c],
            recv_sem=tot_recv.at[sender, c],
            device_id={"lon": jnp.int32(target)},
            device_id_type=MESH,
        )

    def later(act):
        for other in range(1, n_lon):
            pl.when(other > me["lon"])(functools.partial(act, other))

    def earlier(act):
        for other in range(n_lon - 1):
            pl.when(other < me["lon"])(functools.partial(act, other))

    final = STEPS % 2

    def mid_end():
        return pltpu.make_async_copy(
            state.at[final, pl.ds(2, J - 2), rows, levels],
            end.at[pl.ds(1, J - 2)],
            end_sem.at[2, 0],
        )

    def edge_end(which, c):
        plane = 1 if which == 0 else J
        part = pl.ds(pl.multiple_of(PAD + c * CHUNK, CHUNK), CHUNK)
        inner = pl.ds(pl.multiple_of(c * CHUNK, CHUNK), CHUNK)
        return pltpu.make_async_copy(
            state.at[final, plane, rows, part],
            end.at[plane - 1, :, inner],
            end_sem.at[which, c],
        )

    for step in range(STEPS):
        a, b = step % 2, (step + 1) % 2
        last = step == STEPS - 1

        both("lon", lambda side: lon_copy(step, side).start())
        if sizes["lev"] > 1:

            @pl.loop(1, J + 1)
            def _(p):
                lev_out[0, p - 1] = state[a, p, 1 : I + 1, PAD : PAD + 1, :]
                lev_out[1, p - 1] = state[a, p, 1 : I + 1, PAD + K - 1 : PAD + K, :]

        both("lev", lambda side: lev_copy(step, side).start())
        if step == 0:
            for j in range(J):
                load(1, j).wait()
                load(2, j).wait()

        def lon_done(side):
            lon_copy(step, side).wait_send()
            lon_copy(step, side, True).wait_recv()

        def lev_done(side):
            lev_copy(step, side).wait_send()
            lev_copy(step, side, True).wait_recv()
            row = PAD - 1 if side == 0 else PAD + K

            @pl.loop(1, J + 1)
            def _(p):
                state[a, p, 1 : I + 1, row : row + 1, :] = lev_in[a, side, p - 1]

        both("lon", lon_done)
        both("lev", lev_done)

        @pl.loop(2, J)
        def _(p):
            if last:
                tot_mid[p - 2] = lax.fori_loop(
                    1,
                    I + 1,
                    lambda i, total: total + update(step, p, i, PAD, K),
                    jnp.zeros((K, M), jnp.float32),
                )
            else:

                @pl.loop(1, I + 1)
                def _(i):
                    update(step, p, i, PAD, K)

        if last:
            mid_end().start()
            later(lambda other: mid_total(other).start())

        @pl.loop(0, chunks)
        def _(c):
            def ready(side):
                if step > 0:
                    lat_copy(step - 1, side, c).wait_send()
                lat_arrived(step, side, c)

            both("lat", ready)
            start = pl.multiple_of(PAD + c * CHUNK, CHUNK)
            zero = jnp.zeros((CHUNK, M), jnp.float32)

            def row(i, totals):
                return (
                    totals[0] + update(step, 1, i, start, CHUNK),
                    totals[1] + update(step, J, i, start, CHUNK),
                )

            low, high = lax.fori_loop(1, I + 1, row, (zero, zero), unroll=4)
            if last:
                part = pl.ds(pl.multiple_of(c * CHUNK, CHUNK), CHUNK)
                tot_edge[0, part, :] = low
                tot_edge[1, part, :] = high
                later(lambda other: edge_total(other, c).start())
                edge_end(0, c).start()
                edge_end(1, c).start()
            else:
                lat_start(step + 1, c)

    before[...] = jnp.zeros(before.shape, jnp.float32)

    def add_mid(other):
        mid_total(other, other).wait_recv()
        before[1 : J - 1] += mid_in[other]

    def add_edge(other):
        for c in range(chunks):
            edge_total(other, c, other).wait_recv()
        before[0] += edge_in[other, 0]
        before[J - 1] += edge_in[other, 1]

    earlier(add_mid)
    earlier(add_edge)

    for c in range(chunks):
        both("lat", lambda side: lat_copy(STEPS - 1, side, c).wait_send())
        later(lambda other: edge_total(other, c).wait_send())
        edge_end(0, c).wait()
        edge_end(1, c).wait()
    later(lambda other: mid_total(other).wait_send())
    mid_end().wait()


def totals_kernel(scale, x, before, totals, end):
    def row(i, total):
        value = x[0, i]
        total = total + value
        totals[0, i] = total * scale
        end[0, i] = value
        return total

    lax.fori_loop(0, x.shape[1], row, before[0], unroll=4)


def per_device(sizes, initial_state, scaled_diffusivity, scaled_forcing):
    J, I, K, M = initial_state.shape
    chunks = K // CHUNK
    n_lon = sizes["lon"]
    f32 = jnp.float32
    vmem = lambda *shape: pltpu.VMEM(shape, f32)
    sem = lambda *shape: pltpu.SemaphoreType.DMA(shape)
    hbm = pl.BlockSpec(memory_space=pltpu.HBM)
    end, before = pl.pallas_call(
        functools.partial(steps_kernel, sizes),
        out_shape=(
            jax.ShapeDtypeStruct((J, I, K, M), f32),
            jax.ShapeDtypeStruct((J, K, M), f32),
        ),
        in_specs=[hbm] * 3,
        out_specs=(hbm, pl.BlockSpec(memory_space=pltpu.VMEM)),
        scratch_shapes=[
            vmem(2, J + 2, I + 2, K + 2 * PAD, M),
            vmem(J, I, K, M),
            vmem(J, I, K, M),
            vmem(2, J, I, 1, M),
            vmem(2, 2, J, I, 1, M),
            vmem(J - 2, K, M),
            vmem(2, K, M),
            vmem(n_lon, J - 2, K, M),
            vmem(n_lon, 2, K, M),
            sem(2, 2, chunks),
            sem(2, 2, chunks),
            sem(2, 2),
            sem(2, 2),
            sem(2, 2),
            sem(2, 2),
            sem(3, J),
            sem(3, chunks),
            sem(n_lon, chunks + 1),
            sem(n_lon, chunks + 1),
        ],
        compiler_params=pltpu.CompilerParams(
            collective_id=0, has_side_effects=True, vmem_limit_bytes=58 * 2**20
        ),
        name="steps",
    )(initial_state, scaled_diffusivity, scaled_forcing)

    half = K // 2
    block = pl.BlockSpec((1, I, half, M), lambda j, k: (j, 0, k, 0))
    return pl.pallas_call(
        functools.partial(totals_kernel, 1.0 / (I * n_lon)),
        grid=(J, K // half),
        out_shape=(jax.ShapeDtypeStruct((J, I, K, M), f32),) * 2,
        in_specs=[block, pl.BlockSpec((1, half, M), lambda j, k: (j, k, 0))],
        out_specs=(block, block),
        name="totals",
    )(end, before)


def solution(mesh):
    spec = P("lat", "lon", "lev", None)
    return jax.shard_map(
        functools.partial(per_device, dict(mesh.shape)),
        mesh=mesh,
        in_specs=(spec,) * 3,
        out_specs=(spec,) * 2,
        check_vma=False,
    )
```

```python
import functools

import jax
import jax.numpy as jnp
from jax import lax
from jax.experimental import pallas as pl
from jax.experimental.pallas import tpu as pltpu
from jax.sharding import PartitionSpec as P

STEPS = 4
PAD = 8
CHUNK = 8
MESH = pl.DeviceIdType.MESH


def steps_kernel(
    sizes, x, d, f, end, before, state, coef, source,
    lev_out, lev_in, tot_mid, tot_edge, mid_in, edge_in,
    lat_send, lat_recv, lon_send, lon_recv, lev_send, lev_recv,
    load_sem, tot_send, tot_recv,
):
    J, I, K, M = x.shape
    chunks = K // CHUNK
    me = {axis: lax.axis_index(axis) for axis in sizes}
    n_lon = sizes["lon"]
    rows = pl.ds(1, I)
    levels = pl.ds(PAD, K)
    planes = pl.ds(1, J)

    def has(axis, side):
        return me[axis] > 0 if side == 0 else me[axis] < sizes[axis] - 1

    def beside(axis, side):
        return {axis: me[axis] - 1 if side == 0 else me[axis] + 1}

    def both(axis, act):
        if sizes[axis] > 1:
            for side in (0, 1):
                pl.when(has(axis, side))(functools.partial(act, side))

    def load(which, j):
        src, dst = (
            (x.at[j], state.at[0, j + 1, rows, levels]),
            (d.at[j], coef.at[j]),
            (f.at[j], source.at[j]),
        )[which]
        return pltpu.make_async_copy(src, dst, load_sem.at[which, j])

    barrier = pltpu.get_barrier_semaphore()
    count = jnp.int32(n_lon - 1)

    def greet(target):
        pl.semaphore_signal(barrier, inc=1, device_id=target, device_id_type=MESH)

    for axis in ("lat", "lev"):
        both(axis, lambda side, axis=axis: greet(beside(axis, side)))
        if sizes[axis] > 1:
            count = count + has(axis, 0).astype(jnp.int32) + has(axis, 1).astype(jnp.int32)
    for other in range(n_lon):
        pl.when(other != me["lon"])(lambda other=other: greet({"lon": jnp.int32(other)}))
    pl.semaphore_wait(barrier, count)

    def lat_copy(step, side, c):
        slot = step % 2
        part = pl.ds(pl.multiple_of(PAD + c * CHUNK, CHUNK), CHUNK)
        plane, target = (1, J + 1) if side == 0 else (J, 0)
        if step == 0:
            inner = pl.ds(pl.multiple_of(c * CHUNK, CHUNK), CHUNK)
            src = x.at[plane - 1, :, inner]
        else:
            src = state.at[slot, plane, rows, part]
        return pltpu.make_async_remote_copy(
            src_ref=src,
            dst_ref=state.at[slot, target, rows, part],
            send_sem=lat_send.at[slot, side, c],
            recv_sem=lat_recv.at[slot, 1 - side, c],
            device_id=beside("lat", side),
            device_id_type=MESH,
        )

    def lat_arrived(step, side, c):
        slot = step % 2
        part = pl.ds(pl.multiple_of(PAD + c * CHUNK, CHUNK), CHUNK)
        target = 0 if side == 0 else J + 1
        pltpu.make_async_remote_copy(
            src_ref=state.at[slot, target, rows, part],
            dst_ref=state.at[slot, target, rows, part],
            send_sem=lat_send.at[slot, side, c],
            recv_sem=lat_recv.at[slot, side, c],
            device_id=beside("lat", side),
            device_id_type=MESH,
        ).wait_recv()

    def lon_copy(step, side, arriving=False):
        slot = step % 2
        row, target = (1, I + 1) if side == 0 else (I, 0)
        dst = (0 if side == 0 else I + 1) if arriving else target
        return pltpu.make_async_remote_copy(
            src_ref=state.at[slot, planes, row, levels],
            dst_ref=state.at[slot, planes, dst, levels],
            send_sem=lon_send.at[slot, side],
            recv_sem=lon_recv.at[slot, side if arriving else 1 - side],
            device_id=beside("lon", side),
            device_id_type=MESH,
        )

    def lev_copy(step, side, arriving=False):
        slot = step % 2
        landing = side if arriving else 1 - side
        return pltpu.make_async_remote_copy(
            src_ref=lev_out.at[side],
            dst_ref=lev_in.at[slot, landing],
            send_sem=lev_send.at[slot, side],
            recv_sem=lev_recv.at[slot, landing],
            device_id=beside("lev", side),
            device_id_type=MESH,
        )

    def lat_start(step, c):
        both("lat", lambda side: lat_copy(step, side, c).start())

    for c in range(chunks):
        lat_start(0, c)

    for which in range(3):
        for j in range(J):
            load(which, j).start()

    def clear(axis, side):
        for slot in (0, 1):
            if axis == "lat":
                target = 0 if side == 0 else J + 1

                @pl.loop(1, I + 1)
                def _(i):
                    state[slot, target, i, PAD : PAD + K, :] = jnp.zeros((K, M), jnp.float32)
            elif axis == "lon":
                target = 0 if side == 0 else I + 1
                for p in range(1, J + 1):
                    state[slot, p, target, PAD : PAD + K, :] = jnp.zeros((K, M), jnp.float32)
            else:
                target = PAD - 1 if side == 0 else PAD + K

                @pl.loop(1, J + 1)
                def _(p):
                    state[slot, p, 1 : I + 1, target : target + 1, :] = jnp.zeros(
                        (I, 1, M), jnp.float32
                    )

    for axis in ("lat", "lon", "lev"):
        for side in (0, 1):
            pl.when(jnp.logical_not(has(axis, side)))(functools.partial(clear, axis, side))

    for j in range(J):
        load(0, j).wait()

    def update(step, p, i, start, length):
        a, b = step % 2, (step + 1) % 2
        here = pl.ds(start, length)
        inner = pl.ds(start - PAD, length)
        middle = state[a, p, i, here, :]
        spread = (
            (state[a, p - 1, i, here, :] + state[a, p + 1, i, here, :])
            + (state[a, p, i - 1, here, :] + state[a, p, i + 1, here, :])
            + (
                state[a, p, i, pl.ds(start - 1, length), :]
                + state[a, p, i, pl.ds(start + 1, length), :]
            )
            - 6.0 * middle
        )
        new = middle + coef[p - 1, i - 1, inner, :] * spread + source[p - 1, i - 1, inner, :]
        if step == STEPS - 1:
            end[p - 1, i - 1, inner, :] = new
        else:
            state[b, p, i, here, :] = new
        return new

    def mid_total(target, arriving=None):
        sender = me["lon"] if arriving is None else arriving
        return pltpu.make_async_remote_copy(
            src_ref=tot_mid,
            dst_ref=mid_in.at[sender],
            send_sem=tot_send.at[target, chunks],
            recv_sem=tot_recv.at[sender, chunks],
            device_id={"lon": jnp.int32(target)},
            device_id_type=MESH,
        )

    def edge_total(target, c, arriving=None):
        sender = me["lon"] if arriving is None else arriving
        part = pl.ds(pl.multiple_of(c * CHUNK, CHUNK), CHUNK)
        return pltpu.make_async_remote_copy(
            src_ref=tot_edge.at[:, part],
            dst_ref=edge_in.at[sender, :, part],
            send_sem=tot_send.at[target, c],
            recv_sem=tot_recv.at[sender, c],
            device_id={"lon": jnp.int32(target)},
            device_id_type=MESH,
        )

    def later(act):
        for other in range(1, n_lon):
            pl.when(other > me["lon"])(functools.partial(act, other))

    def earlier(act):
        for other in range(n_lon - 1):
            pl.when(other < me["lon"])(functools.partial(act, other))

    def add_mids():
        before[...] = jnp.zeros(before.shape, jnp.float32)

        def add(other):
            mid_total(other, other).wait_recv()
            before[1 : J - 1] += mid_in[other]

        earlier(add)
        for c in range(chunks // 2):
            add_edges(c)

    def add_edges(c):
        part = pl.ds(pl.multiple_of(c * CHUNK, CHUNK), CHUNK)

        def add(other):
            edge_total(other, c, other).wait_recv()
            before[0, part, :] += edge_in[other, 0, part, :]
            before[J - 1, part, :] += edge_in[other, 1, part, :]

        earlier(add)

    for step in range(STEPS):
        a, b = step % 2, (step + 1) % 2
        last = step == STEPS - 1

        both("lon", lambda side: lon_copy(step, side).start())
        if sizes["lev"] > 1:

            @pl.loop(1, J + 1)
            def _(p):
                lev_out[0, p - 1] = state[a, p, 1 : I + 1, PAD : PAD + 1, :]
                lev_out[1, p - 1] = state[a, p, 1 : I + 1, PAD + K - 1 : PAD + K, :]

        both("lev", lambda side: lev_copy(step, side).start())
        if step == 0:
            for j in range(J):
                load(1, j).wait()
                load(2, j).wait()

        def lon_done(side):
            lon_copy(step, side).wait_send()
            lon_copy(step, side, True).wait_recv()

        def lev_done(side):
            lev_copy(step, side).wait_send()
            lev_copy(step, side, True).wait_recv()
            row = PAD - 1 if side == 0 else PAD + K

            @pl.loop(1, J + 1)
            def _(p):
                state[a, p, 1 : I + 1, row : row + 1, :] = lev_in[a, side, p - 1]

        both("lon", lon_done)
        both("lev", lev_done)

        @pl.loop(2, J)
        def _(p):
            if last:
                tot_mid[p - 2] = lax.fori_loop(
                    1,
                    I + 1,
                    lambda i, total: total + update(step, p, i, PAD, K),
                    jnp.zeros((K, M), jnp.float32),
                )
            else:

                @pl.loop(1, I + 1)
                def _(i):
                    update(step, p, i, PAD, K)

        if last:
            later(lambda other: mid_total(other).start())

        @pl.loop(0, chunks)
        def _(c):
            def ready(side):
                if step > 0:
                    lat_copy(step - 1, side, c).wait_send()
                lat_arrived(step, side, c)

            both("lat", ready)
            start = pl.multiple_of(PAD + c * CHUNK, CHUNK)
            zero = jnp.zeros((CHUNK, M), jnp.float32)

            def row(i, totals):
                return (
                    totals[0] + update(step, 1, i, start, CHUNK),
                    totals[1] + update(step, J, i, start, CHUNK),
                )

            low, high = lax.fori_loop(1, I + 1, row, (zero, zero), unroll=4)
            if last:
                part = pl.ds(pl.multiple_of(c * CHUNK, CHUNK), CHUNK)
                tot_edge[0, part, :] = low
                tot_edge[1, part, :] = high
                later(lambda other: edge_total(other, c).start())
                pl.when(c == chunks // 2)(add_mids)

                @pl.when(c > chunks // 2)
                def _():
                    add_edges(c - 1)
            else:
                lat_start(step + 1, c)

    add_edges(chunks - 1)

    for c in range(chunks):
        both("lat", lambda side: lat_copy(STEPS - 1, side, c).wait_send())
        later(lambda other: edge_total(other, c).wait_send())
    later(lambda other: mid_total(other).wait_send())


def totals_kernel(scale, x, before, totals, end, sums, end_sem, sums_sem):
    J, I = x.shape[:2]

    def out(which, j):
        src, dst, sem = ((x, end, end_sem), (sums, totals, sums_sem))[which]
        return pltpu.make_async_copy(src.at[j], dst.at[j], sem.at[j])

    for j in range(J):
        out(0, j).start()

    @pl.loop(0, J)
    def _(j):
        def row(i, total):
            total = total + x[j, i]
            sums[j, i] = total * scale
            return total

        lax.fori_loop(0, I, row, before[j], unroll=4)
        out(1, j).start()

    for j in range(J):
        out(0, j).wait()
        out(1, j).wait()


def per_device(sizes, initial_state, scaled_diffusivity, scaled_forcing):
    J, I, K, M = initial_state.shape
    chunks = K // CHUNK
    n_lon = sizes["lon"]
    f32 = jnp.float32
    vmem = lambda *shape: pltpu.VMEM(shape, f32)
    sem = lambda *shape: pltpu.SemaphoreType.DMA(shape)
    hbm = pl.BlockSpec(memory_space=pltpu.HBM)
    local = pl.BlockSpec(memory_space=pltpu.VMEM)
    end, before = pl.pallas_call(
        functools.partial(steps_kernel, sizes),
        out_shape=(vmem(J, I, K, M), vmem(J, K, M)),
        in_specs=[hbm] * 3,
        out_specs=(local, local),
        scratch_shapes=[
            vmem(2, J + 2, I + 2, K + 2 * PAD, M),
            vmem(J, I, K, M),
            vmem(J, I, K, M),
            vmem(2, J, I, 1, M),
            vmem(2, 2, J, I, 1, M),
            vmem(J - 2, K, M),
            vmem(2, K, M),
            vmem(n_lon, J - 2, K, M),
            vmem(n_lon, 2, K, M),
            sem(2, 2, chunks),
            sem(2, 2, chunks),
            sem(2, 2),
            sem(2, 2),
            sem(2, 2),
            sem(2, 2),
            sem(3, J),
            sem(n_lon, chunks + 1),
            sem(n_lon, chunks + 1),
        ],
        compiler_params=pltpu.CompilerParams(
            collective_id=0, has_side_effects=True, vmem_limit_bytes=48 * 2**20
        ),
        name="steps",
    )(initial_state, scaled_diffusivity, scaled_forcing)

    return pl.pallas_call(
        functools.partial(totals_kernel, 1.0 / (I * n_lon)),
        out_shape=(jax.ShapeDtypeStruct((J, I, K, M), f32),) * 2,
        in_specs=[local, local],
        out_specs=(hbm, hbm),
        scratch_shapes=[vmem(J, I, K, M), sem(J), sem(J)],
        compiler_params=pltpu.CompilerParams(vmem_limit_bytes=20 * 2**20),
        name="totals",
    )(end, before)


def solution(mesh):
    spec = P("lat", "lon", "lev", None)
    return jax.shard_map(
        functools.partial(per_device, dict(mesh.shape)),
        mesh=mesh,
        in_specs=(spec,) * 3,
        out_specs=(spec,) * 2,
        check_vma=False,
    )
```
